512 devices in a mesh: sx: 16 (over z_lo, x, core), sy: 8 (over y), px: 4 (over z_hi).
Axes of the slice: x: 4, y: 8, z: 8 (z_hi: 4, z_lo: 2; z = z_hi * 2 + z_lo), core: 2. Of those that a mesh axis runs over, the one named last changes fastest.
Arguments:
- patterns: bfloat16 [256, 256, 9216], P('sx', 'sy', 'px'), may hold values from -6 to 6
- basis: bfloat16 [9216, 256], P('px', ('sx', 'sy')), may hold values from -0.375 to 0.375
- valid: int32 [256, 256], P('sx', 'sy'), may hold values 0 or 1
- strength: float32 [256, 256], P('sx', 'sy'), may hold values from 0.25 to 2
Outputs:
- denoised: bfloat16 [256, 256, 9216], P('sx', 'sy', 'px')
The draws below stay inside these ranges and needn't reach their ends.
Inputs may be any that keep to these rules, and one draw needn't show every extreme that they name: `valid`: 1 marks an on-sample scan position, 0 an off-sample one.
All inputs are finite; a program needn't handle non-finite values. No bound on the sum of `valid` on one device may be relied on, other than what follows from the above.
Results may differ from the reference program's by a relative error of at most 0.0089.
Values may be sent and summed in bfloat16 or wider, within the bound.
A program may use at most 64 MiB of HBM per device.

```python
import math
import jax
import jax.numpy as jnp
from jax import lax

PIX = 9216
RANK = 256
RADIUS = 3
NX = 256
NY = 256


def touch_ends(entries, own_key, least, top_value):
    longest = entries.shape.index(max(entries.shape))
    spots = []
    for shift in (0, 1):
        where = [jax.random.randint(jax.random.fold_in(own_key, axis), (), 0, length) for axis, length in enumerate(entries.shape)]
        where[longest] = (where[longest] + shift) % entries.shape[longest]
        spots.append(tuple(where))
    return entries.at[spots[0]].set(least).at[spots[1]].set(top_value)


def steps_of(stream_key, dims, split, least, largest):
    def one(axis_at, shards_of):
        steps = jax.random.uniform(jax.random.fold_in(jax.random.fold_in(stream_key, 6), axis_at), (shards_of,), jnp.float32, least / len(split), largest / len(split))
        return jnp.repeat(jnp.exp(steps), dims[axis_at] // shards_of).reshape((-1,) + (1,) * (len(dims) - axis_at - 1))

    level = one(*split[0])
    for cut in split[1:]:
        level = level * one(*cut)
    return level


def gaussian(stream_key, extent, scale, reach, shards=(), dtype=jnp.bfloat16):
    drawn = scale * jax.random.normal(stream_key, extent, jnp.float32)
    if shards:
        drawn = drawn * steps_of(stream_key, extent, shards, -0.22, 0.18)
    return jnp.clip(drawn, -reach, reach).astype(dtype)


def setup_inputs(seed: int = 0) -> dict:
    key_list = jax.random.split(jax.random.key(seed), 5)
    return {
        "patterns": gaussian(key_list[0], (NX, NY, PIX), 1.0, 6.0, ((0, 16), (1, 8), (2, 4))),
        "basis": gaussian(key_list[1], (PIX, RANK), RANK ** -0.5, 0.375, ((0, 4), (1, 128))),
        "valid": touch_ends((jax.random.randint(key_list[2], (NX, NY), 0, 8) < 7).astype(jnp.int32), jax.random.fold_in(key_list[2], 1), 0, 1),
        "strength": jnp.clip(jnp.exp(math.log(2.0) - 2.0794415 * jax.random.uniform(key_list[3], (NX, NY), jnp.float32) ** steps_of(key_list[3], (NX, NY), ((0, 16), (1, 8)), -0.2, 0.2)), 0.25, 2.0),
    }


def neighbour_steps():
    steps = []
    for row_step in range(-RADIUS, RADIUS + 1):
        for col_step in range(-RADIUS, RADIUS + 1):
            if row_step != 0 or col_step != 0:
                steps.append((row_step, col_step))
    return steps


def squared_gaps(center, padded):
    rows, cols = center.shape[0], center.shape[1]
    gaps = []
    for row_step, col_step in neighbour_steps():
        other = padded[RADIUS + row_step:RADIUS + row_step + rows, RADIUS + col_step:RADIUS + col_step + cols]
        differ = center - other
        gaps.append(jnp.sum(differ * differ, axis=-1))
    return jnp.stack(gaps)


def blend(center, padded, mask_pad, gaps, strength):
    rows, cols = center.shape[0], center.shape[1]
    factor = 1.0 / (2.0 * PIX * strength)
    numerator = center
    total = jnp.ones((rows, cols), jnp.float32)
    for index, (row_step, col_step) in enumerate(neighbour_steps()):
        other = padded[RADIUS + row_step:RADIUS + row_step + rows, RADIUS + col_step:RADIUS + col_step + cols]
        mask_other = mask_pad[RADIUS + row_step:RADIUS + row_step + rows, RADIUS + col_step:RADIUS + col_step + cols]
        weight = mask_other * jnp.exp(-gaps[index] * factor)
        numerator = numerator + weight[:, :, None] * other
        total = total + weight
    return numerator / total[:, :, None]


def reference(patterns, basis, valid, strength):
    def project(row_block):
        return jnp.dot(row_block, basis, preferred_element_type=jnp.float32)

    coeffs = lax.map(project, patterns)
    mask_full = valid.astype(jnp.float32)
    padded = jnp.pad(coeffs, ((RADIUS, RADIUS), (RADIUS, RADIUS), (0, 0)))
    mask_pad = jnp.pad(mask_full, ((RADIUS, RADIUS), (RADIUS, RADIUS)))
    gaps = squared_gaps(coeffs, padded)
    average = blend(coeffs, padded, mask_pad, gaps, strength).astype(jnp.bfloat16)

    def rebuild(row_block):
        product = lax.dot_general(row_block, basis, (((1,), (1,)), ((), ())), preferred_element_type=jnp.float32)
        return product.astype(jnp.bfloat16)

    return lax.map(rebuild, average)
```

```python
import functools
import math

import jax
import jax.numpy as jnp
from jax import lax
from jax.experimental import pallas as pl
from jax.experimental.pallas import tpu as pltpu
from jax.sharding import PartitionSpec as P

MESH = pl.DeviceIdType.MESH
RADIUS = 3
NEAR = (2, 4, 2)
FAR = 1e15
OFF = 1e30
EDGE = 4
ROWS = 4


def kernel(
    near, pix_total, patterns_ref, basis_ref, valid_ref, strength_ref,
    avg_ref, gath_ref,
    pat, pieces, stage, own32, part16, arrived, coeff, ext, halo, pack, pick, bias,
    pat_sem, send_sem, recv_sem,
):
    n_z, n_x, n_core = near
    n_sy, n_px = lax.axis_size("sy"), lax.axis_size("px")
    n_sx = n_z * n_x * n_core
    sx, sy, px = lax.axis_index("sx"), lax.axis_index("sy"), lax.axis_index("px")
    core = sx % n_core
    chip_x = (sx // n_core) % n_x
    chip_z = sx // (n_core * n_x)
    depth = basis_ref.shape[0]
    part, rank = part16.shape[1], part16.shape[2]
    cols = part // ROWS

    def at(dz, dx):
        return (((chip_z + dz + n_z) % n_z) * n_x + (chip_x + dx + n_x) % n_x) * n_core + core

    sibling = sx + 1 - 2 * core
    up, down = (sx + 1) % n_sx, (sx + n_sx - 1) % n_sx
    right, left = (sy + 1) % n_sy, (sy + n_sy - 1) % n_sy
    plane = [(dz, dx) for dx in range(n_x) for dz in range(n_z) if (dz, dx) != (0, 0)]

    load = pltpu.make_async_copy(patterns_ref, pat, pat_sem)
    load.start()

    partners = [{"sy": (sy + d) % n_sy} for d in range(1, n_sy)]
    partners += [{"sx": at(dz, dx)} for dz, dx in plane]
    partners += [{"px": (px + d) % n_px} for d in range(1, n_px)]
    partners += [{"sx": sibling}, {"sx": up}, {"sx": down}]
    partners += [{"sx": a, "sy": b} for a in (up, down) for b in (left, right)]

    def device(partner):
        return {"sx": sx, "sy": sy, "px": px, **partner}

    barrier = pltpu.get_barrier_semaphore()
    for partner in partners:
        pl.semaphore_signal(barrier, inc=1, device_id=device(partner), device_id_type=MESH)

    row = lax.broadcasted_iota(jnp.int32, pick.shape, 0)
    col = lax.broadcasted_iota(jnp.int32, pick.shape, 1)
    half = pick.shape[0] // 2
    side = row // half
    wanted = ((row % half) // EDGE) * cols + row % EDGE + side * (cols - EDGE)
    pick[...] = jnp.where(col == wanted, 1.0, 0.0).astype(pick.dtype)

    mine = lax.broadcasted_iota(jnp.int32, bias.shape, 0)
    other = lax.broadcasted_iota(jnp.int32, bias.shape, 1)
    n_mid = (ROWS + 2 * RADIUS) * cols
    n_edge = 3 * 2 * ROWS * EDGE
    edge = other - n_mid
    spot = edge % (ROWS * EDGE)
    side = (edge // (ROWS * EDGE)) % 2
    in_mid = other < n_mid
    other_row = jnp.where(in_mid, other // cols - RADIUS, (edge // (2 * ROWS * EDGE)) * ROWS + spot // EDGE - ROWS)
    other_col = jnp.where(in_mid, other % cols, spot % EDGE + jnp.where(side == 0, cols, -EDGE))
    d_row, d_col = other_row - mine // cols, other_col - mine % cols
    inside = (jnp.abs(d_row) <= RADIUS) & (jnp.abs(d_col) <= RADIUS) & (other < n_mid + n_edge)
    inside = inside & ((d_row != 0) | (d_col != 0))
    bias[...] = jnp.where(inside, 0.0, OFF)

    pl.semaphore_wait(barrier, len(partners))

    sent = []

    def send(src, dst, partner):
        k = len(sent)
        copy = pltpu.make_async_remote_copy(
            src_ref=src, dst_ref=dst, send_sem=send_sem.at[k], recv_sem=recv_sem.at[k],
            device_id=device(partner), device_id_type=MESH,
        )
        copy.start()
        sent.append(copy)
        return copy

    order = sorted(range(1, n_sy), key=lambda d: -min(d, n_sy - d))
    along = [send(basis_ref, pieces.at[sy], {"sy": (sy + d) % n_sy}) for d in order]
    pieces[pl.ds(sy, 1)] = basis_ref[...][None]
    for copy in along:
        copy.wait_recv()
    for y in range(n_sy):
        stage[depth * y:depth * (y + 1), :] = pieces[y].astype(jnp.float32)
    gath_ref[sx] = stage[...].astype(gath_ref.dtype)

    across = [(dz, dx, send(gath_ref.at[sx], gath_ref.at[sx], {"sx": at(dz, dx)})) for dz, dx in plane]
    passed = [send(gath_ref.at[sx], gath_ref.at[sx], {"sx": sibling})]
    for dz, dx, copy in across:
        copy.wait_recv()
        tile = at(-dz, -dx)
        passed.append(send(gath_ref.at[tile], gath_ref.at[tile], {"sx": sibling}))
    load.wait()
    for copy in passed:
        copy.wait_recv()

    whole = gath_ref[...].reshape(rank, gath_ref.shape[2])

    def project(which):
        block = pat[pl.ds(pl.multiple_of(which * part, part), part), :]
        return lax.dot_general(block, whole, (((1,), (1,)), ((), ())), preferred_element_type=jnp.float32)

    reduce = []
    far_first = sorted(range(1, n_px), key=lambda d: -min(d, n_px - d))
    for d in far_first:
        part16[d] = project((px + d) % n_px).astype(part16.dtype)
        reduce.append(send(part16.at[d], arrived.at[d], {"px": (px + d) % n_px}))
    own32[...] = project(px)
    for copy in reduce:
        copy.wait_recv()
    total = own32[...]
    for d in range(1, n_px):
        total = total + arrived[d].astype(jnp.float32)
    coeff[px] = total.astype(coeff.dtype)
    spread = [send(coeff.at[px], coeff.at[px], {"px": (px + d) % n_px}) for d in far_first]
    for copy in spread:
        copy.wait_recv()

    valid = jnp.transpose(valid_ref[...].astype(jnp.float32))
    n_rows = n_px * ROWS
    for r in range(n_rows):
        values = coeff[r // ROWS, (r % ROWS) * cols:(r % ROWS + 1) * cols, :].astype(jnp.float32)
        ext[RADIUS + r] = jnp.where(valid[:, r:r + 1] > 0.5, values, FAR).astype(ext.dtype)
    tile = ext[RADIUS:RADIUS + n_rows].reshape(n_rows * cols, rank)
    edges = jnp.dot(pick[...], tile, preferred_element_type=jnp.float32).astype(pack.dtype)
    pack[...] = edges.reshape(pack.shape)
    last = n_px - 1
    swap = [
        send(pack.at[0, 0], halo.at[n_px + 1, 0], {"sx": down, "sy": left}),
        send(pack.at[0, last], halo.at[0, 0], {"sx": up, "sy": left}),
        send(pack.at[1, 0], halo.at[n_px + 1, 1], {"sx": down, "sy": right}),
        send(pack.at[1, last], halo.at[0, 1], {"sx": up, "sy": right}),
        send(ext.at[pl.ds(RADIUS, RADIUS)], ext.at[pl.ds(RADIUS + n_rows, RADIUS)], {"sx": down}),
        send(ext.at[pl.ds(n_rows, RADIUS)], ext.at[pl.ds(0, RADIUS)], {"sx": up}),
        send(pack.at[0], halo.at[pl.ds(1, n_px), 0], {"sy": left}),
        send(pack.at[1], halo.at[pl.ds(1, n_px), 1], {"sy": right}),
    ]
    for copy in swap:
        copy.wait_recv()

    @pl.when(sx == 0)
    def _():
        ext[0:RADIUS] = jnp.full((RADIUS, cols, rank), FAR, ext.dtype)
        halo[0] = jnp.full(halo.shape[1:], FAR, halo.dtype)

    @pl.when(sx == n_sx - 1)
    def _():
        ext[RADIUS + n_rows:] = jnp.full((RADIUS, cols, rank), FAR, ext.dtype)
        halo[n_px + 1] = jnp.full(halo.shape[1:], FAR, halo.dtype)

    @pl.when(sy == 0)
    def _():
        halo[:, 1] = jnp.full((n_px + 2,) + halo.shape[2:], FAR, halo.dtype)

    @pl.when(sy == n_sy - 1)
    def _():
        halo[:, 0] = jnp.full((n_px + 2,) + halo.shape[2:], FAR, halo.dtype)

    factor = (math.log2(math.e) / (2.0 * pix_total)) / jnp.transpose(strength_ref[...])
    n_pad = bias.shape[1] - n_mid - n_edge
    for b in range(n_px):
        center = coeff[b]
        center32 = center.astype(jnp.float32)
        around = jnp.concatenate(
            [
                ext[ROWS * b:ROWS * b + ROWS + 2 * RADIUS].reshape(n_mid, rank),
                halo[b:b + 3].reshape(n_edge, rank),
                jnp.zeros((n_pad, rank), ext.dtype),
            ],
            axis=0,
        )
        around32 = around.astype(jnp.float32)
        inner = lax.dot_general(center, around, (((1,), (1,)), ((), ())), preferred_element_type=jnp.float32)
        size_other = lax.dot_general(
            jnp.ones((8, rank), jnp.float32), around32 * around32, (((1,), (1,)), ((), ())),
            precision=lax.Precision.HIGHEST, preferred_element_type=jnp.float32,
        )[0:1]
        size_mine = jnp.sum(center32 * center32, axis=1, keepdims=True)
        scale = jnp.concatenate([factor[:, ROWS * b + r:ROWS * b + r + 1] for r in range(ROWS)], axis=0)
        gap = jnp.maximum(size_mine + size_other - 2.0 * inner, 0.0)
        weight = jnp.exp2(-(gap * scale + bias[...])).astype(jnp.bfloat16)
        summed = jnp.dot(weight, around, preferred_element_type=jnp.float32)
        mass = jnp.sum(weight.astype(jnp.float32), axis=1, keepdims=True)
        avg_ref[b] = ((center32 + summed) / (1.0 + mass)).astype(avg_ref.dtype)

    for copy in sent:
        copy.wait_send()


def on_device(near, pix_total, patterns, basis, valid, strength):
    cells_x, cells_y, pixels = patterns.shape
    n_sx, n_sy, n_px = (lax.axis_size(name) for name in ("sx", "sy", "px"))
    depth = basis.shape[1]
    rank = depth * n_sx * n_sy
    part = cells_x * cells_y // n_px
    bf16, f32 = jnp.bfloat16, jnp.float32
    n_copies = (n_sy - 1) + 2 * (n_sx // 2 - 1) + 1 + 2 * (n_px - 1) + 8
    n_around = (ROWS + 2 * RADIUS) * cells_y + 6 * ROWS * EDGE
    n_around = -(-n_around // 128) * 128
    vmem = pl.BlockSpec(memory_space=pltpu.VMEM)
    avg, gathered = pl.pallas_call(
        functools.partial(kernel, near, pix_total),
        out_shape=(
            jax.ShapeDtypeStruct((n_px, part, rank), bf16),
            jax.ShapeDtypeStruct((n_sx, depth * n_sy, pixels), bf16),
        ),
        in_specs=[pl.BlockSpec(memory_space=pl.ANY), vmem, vmem, vmem],
        out_specs=(vmem, vmem),
        scratch_shapes=[
            pltpu.VMEM((n_px * part, pixels), bf16),
            pltpu.VMEM((n_sy, depth, pixels), bf16),
            pltpu.VMEM((n_sy * depth, pixels), f32),
            pltpu.VMEM((part, rank), f32),
            pltpu.VMEM((n_px, part, rank), bf16),
            pltpu.VMEM((n_px, part, rank), bf16),
            pltpu.VMEM((n_px, part, rank), bf16),
            pltpu.VMEM((cells_x + 2 * RADIUS, cells_y, rank), bf16),
            pltpu.VMEM((n_px + 2, 2, ROWS * EDGE, rank), bf16),
            pltpu.VMEM((2, n_px, ROWS * EDGE, rank), bf16),
            pltpu.VMEM((2 * cells_x * EDGE, cells_x * cells_y), bf16),
            pltpu.VMEM((part, n_around), f32),
            pltpu.SemaphoreType.DMA,
            pltpu.SemaphoreType.DMA((n_copies,)),
            pltpu.SemaphoreType.DMA((n_copies,)),
        ],
        compiler_params=pltpu.CompilerParams(collective_id=0, has_side_effects=True),
    )(patterns.reshape(cells_x * cells_y, pixels), basis.T, valid, strength)
    rebuilt = jnp.dot(
        avg.reshape(cells_x * cells_y, rank), gathered.reshape(rank, pixels), preferred_element_type=f32
    )
    return rebuilt.astype(bf16).reshape(cells_x, cells_y, pixels)


def solution(mesh, near=NEAR, pix_total=9216):
    return jax.shard_map(
        functools.partial(on_device, near, pix_total),
        mesh=mesh,
        in_specs=(P("sx", "sy", "px"), P("px", ("sx", "sy")), P("sx", "sy"), P("sx", "sy")),
        out_specs=P("sx", "sy", "px"),
        check_vma=False,
    )
```

```python
import functools
import math

import jax
import jax.numpy as jnp
from jax import lax
from jax.experimental import pallas as pl
from jax.experimental.pallas import tpu as pltpu
from jax.sharding import PartitionSpec as P

MESH = pl.DeviceIdType.MESH
RADIUS = 3
NEAR = (2, 4, 2)
FAR = 1e15
OFF = 1e30
EDGE = 4
ROWS = 4
NT = (((1,), (1,)), ((), ()))


def across(column):
    n = column.shape[0]
    eye = lax.broadcasted_iota(jnp.int32, (n, n), 0) == lax.broadcasted_iota(jnp.int32, (n, n), 1)
    return jnp.sum(jnp.where(eye, column, 0.0), axis=0, keepdims=True)


def norms(values):
    wide = values.astype(jnp.float32)
    return jnp.sum(wide * wide, axis=1, keepdims=True)


def outside(d_row, d_col, known):
    near = (jnp.abs(d_row) <= RADIUS) & (jnp.abs(d_col) <= RADIUS) & known
    return jnp.where(near & ((d_row != 0) | (d_col != 0)), 0.0, OFF)


def weigh(center, size, scale, around, sizes, bias):
    inner = lax.dot_general(center, around, NT, preferred_element_type=jnp.float32)
    gap = jnp.maximum(size + sizes - 2.0 * inner, 0.0)
    weight = jnp.exp2(-(gap * scale + bias)).astype(jnp.bfloat16)
    summed = jnp.dot(weight, around, preferred_element_type=jnp.float32)
    return summed, jnp.sum(weight.astype(jnp.float32), axis=1, keepdims=True)


def kernel(
    near, pix_total, patterns_ref, basis_ref, valid_ref, strength_ref,
    avg_ref, gath_ref,
    pat, pieces, own32, part16, arrived, coeff, seen, rim, halo, pack, pick, bias, bias_top, bias_low, bias_side,
    size_col, size_row, around_num, around_mass, valid_v, strength_v,
    pat_sem, basis_sem, map_sem, send_sem, recv_sem,
):
    n_z, n_x, n_core = near
    n_sy, n_px = lax.axis_size("sy"), lax.axis_size("px")
    n_sx = n_z * n_x * n_core
    sx, sy, px = lax.axis_index("sx"), lax.axis_index("sy"), lax.axis_index("px")
    core = sx % n_core
    chip_x = (sx // n_core) % n_x
    chip_z = sx // (n_core * n_x)
    depth, pixels = pieces.shape[2], pieces.shape[3]
    part, rank = own32.shape
    cols = part // ROWS
    n_rows = n_px * ROWS
    pad = RADIUS * cols
    f32, bf16 = jnp.float32, jnp.bfloat16

    def at(dz, dx):
        return (((chip_z + dz + n_z) % n_z) * n_x + (chip_x + dx + n_x) % n_x) * n_core + core

    sibling = sx + 1 - 2 * core
    up, down = (sx + 1) % n_sx, (sx + n_sx - 1) % n_sx
    right, left = (sy + 1) % n_sy, (sy + n_sy - 1) % n_sy
    hops = [min(d, n_x - d) for d in range(n_x)]
    plane = sorted(((dz, dx) for dx in range(n_x) for dz in range(n_z) if (dz, dx) != (0, 0)), key=lambda c: c[0] + hops[c[1]])

    load_basis = pltpu.make_async_copy(basis_ref, pieces.at[sx, sy], basis_sem)
    load_basis.start()
    load_maps = [
        pltpu.make_async_copy(valid_ref, valid_v, map_sem.at[0]),
        pltpu.make_async_copy(strength_ref, strength_v, map_sem.at[1]),
    ]
    for copy in load_maps:
        copy.start()
    load = pltpu.make_async_copy(patterns_ref, pat, pat_sem)
    load.start()

    partners = [{"sy": (sy + d) % n_sy} for d in range(1, n_sy)]
    partners += [{"sx": at(dz, dx)} for dz, dx in plane]
    partners += [{"px": (px + d) % n_px} for d in range(1, n_px)]
    partners += [{"sx": sibling}, {"sx": up}, {"sx": down}]
    partners += [{"sx": a, "sy": b} for a in (up, down) for b in (left, right)]

    def device(partner):
        return {"sx": sx, "sy": sy, "px": px, **partner}

    barrier = pltpu.get_barrier_semaphore()
    for partner in partners:
        pl.semaphore_signal(barrier, inc=1, device_id=device(partner), device_id_type=MESH)

    row = lax.broadcasted_iota(jnp.int32, pick.shape, 0)
    col = lax.broadcasted_iota(jnp.int32, pick.shape, 1)
    side, spot = row // (ROWS * EDGE), row % (ROWS * EDGE)
    pick[...] = jnp.where(col == (spot // EDGE) * cols + spot % EDGE + side * (cols - EDGE), 1.0, 0.0).astype(bf16)

    mine = lax.broadcasted_iota(jnp.int32, (part, 128), 0)
    lane = lax.broadcasted_iota(jnp.int32, (part, 128), 1)
    my_row, my_col = mine // cols, mine % cols
    n_mid = (ROWS + 2 * RADIUS) * cols
    n_side = 3 * 2 * ROWS * EDGE
    for k in range(bias.shape[1] // 128):
        spot = lane + 128 * k
        bias[:, 128 * k:128 * (k + 1)] = outside(spot // cols - RADIUS - my_row, spot % cols - my_col, spot < n_mid)
    spot = lane % (ROWS * EDGE)
    side_row = (lane // (2 * ROWS * EDGE)) * ROWS + spot // EDGE - ROWS
    side_col = spot % EDGE + jnp.where((lane // (ROWS * EDGE)) % 2 == 0, cols, -EDGE)
    bias_side[...] = outside(side_row - my_row, side_col - my_col, lane < n_side)
    bias_top[...] = outside(lane // cols - RADIUS - my_row, lane % cols - my_col, lane < pad)
    bias_low[...] = outside(lane // cols + ROWS - my_row, lane % cols - my_col, lane < pad)
    coeff[0:pad] = jnp.zeros((pad, rank), bf16)
    coeff[pad + n_px * part:] = jnp.zeros((coeff.shape[0] - pad - n_px * part, rank), bf16)
    size_row[...] = jnp.full(size_row.shape, OFF, f32)

    load_basis.wait()
    pl.semaphore_wait(barrier, len(partners))

    sent = []
    n_send = [0]

    def remote(src, dst, partner, k):
        return pltpu.make_async_remote_copy(
            src_ref=src, dst_ref=dst, send_sem=send_sem.at[k], recv_sem=recv_sem.at[k],
            device_id=device(partner), device_id_type=MESH,
        )

    def fresh():
        n_send[0] += 1
        return n_send[0] - 1

    def send(src, dst, partner):
        copy = remote(src, dst, partner, fresh())
        copy.start()
        sent.append(copy)
        return copy

    order = sorted(range(1, n_sy), key=lambda d: -min(d, n_sy - d))
    along = {d: send(pieces.at[sx, sy], pieces.at[sx, sy], {"sy": (sy + d) % n_sy}) for d in order}
    plane_sem = {c: fresh() for c in plane}

    def to_plane(y):
        for dz, dx in plane:
            remote(pieces.at[sx, y], pieces.at[sx, y], {"sx": at(dz, dx)}, plane_sem[dz, dx]).start()

    to_plane(sy)
    for d in reversed(order):
        along[d].wait_recv()
        to_plane((sy + n_sy - d) % n_sy)

    passed = [(sx, send(pieces.at[sx], pieces.at[sx], {"sx": sibling}))]
    merge_tile(pieces, gath_ref, sx)
    for dz, dx in plane:
        tile = at(-dz, -dx)
        remote(pieces.at[tile], pieces.at[tile], {"sx": at(dz, dx)}, plane_sem[dz, dx]).wait_recv()
        passed.append((tile, send(pieces.at[tile], pieces.at[tile], {"sx": sibling})))
        merge_tile(pieces, gath_ref, tile)
    for tile, copy in passed:
        copy.wait_recv()
        merge_tile(pieces, gath_ref, tile + 1 - 2 * core)
    load.wait()

    whole = gath_ref[...].reshape(rank, pixels)

    def project(which):
        block = pat[pl.ds(pl.multiple_of(which * part, part), part), :]
        return lax.dot_general(block, whole, NT, preferred_element_type=f32)

    reduce = []
    far_first = sorted(range(1, n_px), key=lambda d: -min(d, n_px - d))
    for d in far_first:
        part16[d] = project((px + d) % n_px).astype(bf16)
        reduce.append(send(part16.at[d], arrived.at[d], {"px": (px + d) % n_px}))
    own32[...] = project(px)
    for copy in load_maps:
        copy.wait()
    valid = jnp.transpose(valid_v[...].astype(f32))
    factor = (math.log2(math.e) / (2.0 * pix_total)) / jnp.transpose(strength_v[...])
    for b in range(n_px):
        for r in range(ROWS):
            size_col[b, cols * r:cols * (r + 1), 0:1] = valid[:, ROWS * b + r:ROWS * b + r + 1]
            size_col[b, cols * r:cols * (r + 1), 1:2] = factor[:, ROWS * b + r:ROWS * b + r + 1]
    for copy in reduce:
        copy.wait_recv()
    total = own32[...]
    for d in range(1, n_px):
        total = total + arrived[d].astype(f32)

    def slot(which):
        return coeff.at[pl.ds(pl.multiple_of(pad + which * part, ROWS * EDGE), part)]

    slot(px)[...] = total.astype(bf16)
    spread = [(d, send(slot(px), slot(px), {"px": (px + d) % n_px})) for d in far_first]

    def look(which):
        values = slot(which)[...]
        on = size_col[which, :, 0:1] > 0.5
        size = norms(values)
        size_col[which, :, 2:3] = size
        shown = jnp.where(on, values.astype(f32), FAR).astype(bf16)
        seen[which] = shown
        edges = jnp.dot(pick[...], shown, preferred_element_type=f32).astype(bf16)
        pack[0, which] = edges[:ROWS * EDGE]
        pack[1, which] = edges[ROWS * EDGE:]

    look(px)
    for d, copy in reversed(spread):
        copy.wait_recv()
        look((px + n_px - d) % n_px)
    last = n_px - 1
    swap = [
        send(seen.at[0, pl.ds(0, pad)], rim.at[1], {"sx": down}),
        send(seen.at[last, pl.ds(part - pad, pad)], rim.at[0], {"sx": up}),
        send(pack.at[0, 0], halo.at[n_px + 1, 0], {"sx": down, "sy": left}),
        send(pack.at[0, last], halo.at[0, 0], {"sx": up, "sy": left}),
        send(pack.at[1, 0], halo.at[n_px + 1, 1], {"sx": down, "sy": right}),
        send(pack.at[1, last], halo.at[0, 1], {"sx": up, "sy": right}),
        send(pack.at[0], halo.at[pl.ds(1, n_px), 0], {"sy": left}),
        send(pack.at[1], halo.at[pl.ds(1, n_px), 1], {"sy": right}),
    ]

    for b in range(n_px):
        column = jnp.where(size_col[b, :, 0:1] > 0.5, size_col[b, :, 2:3], OFF)
        size_row[0:1, 128 * b + 128:128 * b + 128 + part] = across(column)
    n_wide = bias.shape[1]
    for b in range(n_px):
        center = coeff[pad + part * b:pad + part * (b + 1)]
        lanes = 128 - pad + part * b
        sizes = jnp.concatenate([size_row[0:1, lanes:lanes + n_wide]], axis=1)
        around_num[b], around_mass[b] = weigh(
            center, size_col[b, :, 2:3], size_col[b, :, 1:2], coeff[part * b:part * b + n_wide], sizes, bias[...]
        )

    for copy in swap:
        copy.wait_recv()

    @pl.when(sx == 0)
    def _():
        rim[0] = jnp.full(rim.shape[1:], FAR, bf16)
        halo[0] = jnp.full(halo.shape[1:], FAR, bf16)

    @pl.when(sx == n_sx - 1)
    def _():
        rim[1] = jnp.full(rim.shape[1:], FAR, bf16)
        halo[n_px + 1] = jnp.full(halo.shape[1:], FAR, bf16)

    @pl.when(sy == 0)
    def _():
        halo[:, 1] = jnp.full((n_px + 2,) + halo.shape[2:], FAR, bf16)

    @pl.when(sy == n_sy - 1)
    def _():
        halo[:, 0] = jnp.full((n_px + 2,) + halo.shape[2:], FAR, bf16)

    def filled(values):
        return jnp.concatenate([values, jnp.zeros((128 - values.shape[0], rank), bf16)], axis=0)

    for b in range(n_px):
        center = coeff[pad + part * b:pad + part * (b + 1)]
        around, outer = [filled(halo[b:b + 3].reshape(n_side, rank))], [bias_side[...]]
        if b == 0:
            around, outer = around + [filled(rim[0])], outer + [bias_top[...]]
        if b == last:
            around, outer = around + [filled(rim[1])], outer + [bias_low[...]]
        sizes = jnp.concatenate([across(norms(values)) for values in around], axis=1)
        summed, mass = weigh(
            center, size_col[b, :, 2:3], size_col[b, :, 1:2],
            jnp.concatenate(around, axis=0), sizes, jnp.concatenate(outer, axis=1),
        )
        summed = center.astype(f32) + around_num[b] + summed
        avg_ref[b] = (summed / (1.0 + around_mass[b] + mass)).astype(bf16)

    for dz, dx in plane:
        remote(pieces.at[sx], pieces.at[sx], {"sx": at(dz, dx)}, plane_sem[dz, dx]).wait_send()
    for copy in sent:
        copy.wait_send()


def merge_tile(pieces, gath_ref, tile):
    gath_ref[tile] = pieces[tile].reshape(gath_ref.shape[1:])


def on_device(near, pix_total, patterns, basis, valid, strength):
    cells_x, cells_y, pixels = patterns.shape
    n_sx, n_sy, n_px = (lax.axis_size(name) for name in ("sx", "sy", "px"))
    depth = basis.shape[1]
    rank = depth * n_sx * n_sy
    part = cells_x * cells_y // n_px
    pad = RADIUS * cells_y
    bf16, f32 = jnp.bfloat16, jnp.float32
    n_copies = (n_sy - 1) + 2 * (n_sx // 2 - 1) + 1 + 2 * (n_px - 1) + 8
    n_wide = -(-(ROWS + 2 * RADIUS) * cells_y // 128) * 128
    vmem, hbm = pl.BlockSpec(memory_space=pltpu.VMEM), pl.BlockSpec(memory_space=pltpu.HBM)
    avg, gathered = pl.pallas_call(
        functools.partial(kernel, near, pix_total),
        out_shape=(
            jax.ShapeDtypeStruct((n_px, part, rank), bf16),
            jax.ShapeDtypeStruct((n_sx, depth * n_sy, pixels), bf16),
        ),
        in_specs=[hbm, hbm, hbm, hbm],
        out_specs=(vmem, vmem),
        scratch_shapes=[
            pltpu.VMEM((n_px * part, pixels), bf16),
            pltpu.VMEM((n_sx, n_sy, depth, pixels), bf16),
            pltpu.VMEM((part, rank), f32),
            pltpu.VMEM((n_px, part, rank), bf16),
            pltpu.VMEM((n_px, part, rank), bf16),
            pltpu.VMEM((n_wide + (n_px - 1) * part, rank), bf16),
            pltpu.VMEM((n_px, part, rank), bf16),
            pltpu.VMEM((2, pad, rank), bf16),
            pltpu.VMEM((n_px + 2, 2, ROWS * EDGE, rank), bf16),
            pltpu.VMEM((2, n_px, ROWS * EDGE, rank), bf16),
            pltpu.VMEM((2 * ROWS * EDGE, part), bf16),
            pltpu.VMEM((part, n_wide), f32),
            pltpu.VMEM((part, 128), f32),
            pltpu.VMEM((part, 128), f32),
            pltpu.VMEM((part, 128), f32),
            pltpu.VMEM((n_px, part, 128), f32),
            pltpu.VMEM((8, 128 + n_px * part + 512), f32),
            pltpu.VMEM((n_px, part, rank), f32),
            pltpu.VMEM((n_px, part, 1), f32),
            pltpu.VMEM(valid.shape, valid.dtype),
            pltpu.VMEM(strength.shape, strength.dtype),
            pltpu.SemaphoreType.DMA,
            pltpu.SemaphoreType.DMA,
            pltpu.SemaphoreType.DMA((2,)),
            pltpu.SemaphoreType.DMA((n_copies,)),
            pltpu.SemaphoreType.DMA((n_copies,)),
        ],
        compiler_params=pltpu.CompilerParams(collective_id=0, has_side_effects=True, vmem_limit_bytes=30 * 2**20),
    )(*[pltpu.with_memory_space_constraint(a, pltpu.HBM) for a in (patterns.reshape(cells_x * cells_y, pixels), basis.T, valid, strength)])
    rebuilt = jnp.dot(
        avg.reshape(cells_x * cells_y, rank), gathered.reshape(rank, pixels), preferred_element_type=f32
    )
    return rebuilt.astype(bf16).reshape(cells_x, cells_y, pixels)


def solution(mesh, near=NEAR, pix_total=9216):
    return jax.shard_map(
        functools.partial(on_device, near, pix_total),
        mesh=mesh,
        in_specs=(P("sx", "sy", "px"), P("px", ("sx", "sy")), P("sx", "sy"), P("sx", "sy")),
        out_specs=P("sx", "sy", "px"),
        check_vma=False,
    )
```

```python
import functools
import math

import jax
import jax.numpy as jnp
from jax import lax
from jax.experimental import pallas as pl
from jax.experimental.pallas import tpu as pltpu
from jax.sharding import PartitionSpec as P

MESH = pl.DeviceIdType.MESH
RADIUS = 3
NEAR = (2, 4, 2)
FAR = 1e15
OFF = 1e30
EDGE = 4
LAG = 3
ROWS = 4
NT = (((1,), (1,)), ((), ()))


def across(column):
    n = column.shape[0]
    eye = lax.broadcasted_iota(jnp.int32, (n, n), 0) == lax.broadcasted_iota(jnp.int32, (n, n), 1)
    return jnp.sum(jnp.where(eye, column, 0.0), axis=0, keepdims=True)


def norms(values):
    wide = values.astype(jnp.float32)
    return jnp.sum(wide * wide, axis=1, keepdims=True)


def outside(d_row, d_col, known):
    near = (jnp.abs(d_row) <= RADIUS) & (jnp.abs(d_col) <= RADIUS) & known
    return jnp.where(near & ((d_row != 0) | (d_col != 0)), 0.0, OFF)


def weigh(center, size, scale, around, sizes, bias):
    inner = lax.dot_general(center, around, NT, preferred_element_type=jnp.float32)
    gap = jnp.maximum(size + sizes - 2.0 * inner, 0.0)
    weight = jnp.exp2(-(gap * scale + bias)).astype(jnp.bfloat16)
    summed = jnp.dot(weight, around, preferred_element_type=jnp.float32)
    return summed, jnp.sum(weight.astype(jnp.float32), axis=1, keepdims=True)


def kernel(
    near, pix_total, patterns_ref, basis_ref, valid_ref, strength_ref,
    avg_ref, gath_ref,
    pat, pieces, own32, part16, arrived, coeff, seen, rim, halo, pack, pick, bias, bias_top, bias_low, bias_side,
    size_col, size_row, around_num, around_mass, valid_v, strength_v,
    pat_sem, basis_sem, map_sem, send_sem, recv_sem,
):
    n_z, n_x, n_core = near
    n_sy, n_px = lax.axis_size("sy"), lax.axis_size("px")
    n_sx = n_z * n_x * n_core
    sx, sy, px = lax.axis_index("sx"), lax.axis_index("sy"), lax.axis_index("px")
    core = sx % n_core
    chip_x = (sx // n_core) % n_x
    chip_z = sx // (n_core * n_x)
    depth, pixels = pieces.shape[2], pieces.shape[3]
    part, half = own32.shape[1:]
    rank = n_z * half
    cols = part // ROWS
    n_rows = n_px * ROWS
    pad = RADIUS * cols
    f32, bf16 = jnp.float32, jnp.bfloat16

    def at(dz, dx):
        return (((chip_z + dz + n_z) % n_z) * n_x + (chip_x + dx + n_x) % n_x) * n_core + core

    sibling = sx + 1 - 2 * core
    up, down = (sx + 1) % n_sx, (sx + n_sx - 1) % n_sx
    right, left = (sy + 1) % n_sy, (sy + n_sy - 1) % n_sy
    hops = [min(d, n_x - d) for d in range(n_x)]
    plane = sorted(((dz, dx) for dx in range(n_x) for dz in range(n_z) if (dz, dx) != (0, 0)), key=lambda c: c[0] + hops[c[1]])

    load_basis = pltpu.make_async_copy(basis_ref, pieces.at[sx, sy], basis_sem)
    load_basis.start()
    load_maps = [
        pltpu.make_async_copy(valid_ref, valid_v, map_sem.at[0]),
        pltpu.make_async_copy(strength_ref, strength_v, map_sem.at[1]),
    ]
    for copy in load_maps:
        copy.start()
    load = pltpu.make_async_copy(patterns_ref, pat, pat_sem)
    load.start()

    partners = [{"sy": (sy + d) % n_sy} for d in range(1, n_sy)]
    partners += [{"sx": at(dz, dx)} for dz, dx in plane]
    partners += [{"px": (px + d) % n_px} for d in range(1, n_px)]
    partners += [{"sx": sibling}, {"sx": up}, {"sx": down}]
    partners += [{"sx": a, "sy": b} for a in (up, down) for b in (left, right)]

    def device(partner):
        return {"sx": sx, "sy": sy, "px": px, **partner}

    barrier = pltpu.get_barrier_semaphore()
    for partner in partners:
        pl.semaphore_signal(barrier, inc=1, device_id=device(partner), device_id_type=MESH)

    row = lax.broadcasted_iota(jnp.int32, pick.shape, 0)
    col = lax.broadcasted_iota(jnp.int32, pick.shape, 1)
    side, spot = row // (ROWS * EDGE), row % (ROWS * EDGE)
    pick[...] = jnp.where(col == (spot // EDGE) * cols + spot % EDGE + side * (cols - EDGE), 1.0, 0.0).astype(bf16)

    mine = lax.broadcasted_iota(jnp.int32, (part, 128), 0)
    lane = lax.broadcasted_iota(jnp.int32, (part, 128), 1)
    my_row, my_col = mine // cols, mine % cols
    n_mid = (ROWS + 2 * RADIUS) * cols
    n_side = 3 * 2 * ROWS * EDGE
    for k in range(bias.shape[1] // 128):
        spot = lane + 128 * k
        bias[:, 128 * k:128 * (k + 1)] = outside(spot // cols - RADIUS - my_row, spot % cols - my_col, spot < n_mid)
    spot = lane % (ROWS * EDGE)
    side_row = (lane // (2 * ROWS * EDGE)) * ROWS + spot // EDGE - ROWS
    side_col = spot % EDGE + jnp.where((lane // (ROWS * EDGE)) % 2 == 0, cols, -EDGE)
    bias_side[...] = outside(side_row - my_row, side_col - my_col, lane < n_side)
    bias_top[...] = outside(lane // cols - RADIUS - my_row, lane % cols - my_col, lane < pad)
    bias_low[...] = outside(lane // cols + ROWS - my_row, lane % cols - my_col, lane < pad)
    n_tail = coeff.shape[1] - pad - n_px * part
    coeff[:, 0:pad] = jnp.zeros((n_z, pad, half), bf16)
    coeff[:, pad + n_px * part:] = jnp.zeros((n_z, n_tail, half), bf16)
    size_row[...] = jnp.full(size_row.shape, OFF, f32)

    load_basis.wait()
    pl.semaphore_wait(barrier, len(partners))

    sent = []
    n_send = [0]

    def remote(src, dst, partner, k):
        return pltpu.make_async_remote_copy(
            src_ref=src, dst_ref=dst, send_sem=send_sem.at[k], recv_sem=recv_sem.at[k],
            device_id=device(partner), device_id_type=MESH,
        )

    def fresh():
        n_send[0] += 1
        return n_send[0] - 1

    def send(src, dst, partner):
        copy = remote(src, dst, partner, fresh())
        copy.start()
        sent.append(copy)
        return copy

    order = sorted(range(1, n_sy), key=lambda d: -min(d, n_sy - d))
    along = {d: send(pieces.at[sx, sy], pieces.at[sx, sy], {"sy": (sy + d) % n_sy}) for d in order}
    plane_sem = {c: fresh() for c in plane}

    def to_plane(y, targets):
        for dz, dx in targets:
            remote(pieces.at[sx, y], pieces.at[sx, y], {"sx": at(dz, dx)}, plane_sem[dz, dx]).start()

    soon = [c for c in plane if c[0] == 0 or c[1] == 0]
    later = [c for c in plane if c not in soon]
    held = []
    for d in [0] + order[::-1]:
        if d:
            along[d].wait_recv()
        y = (sy + n_sy - d) % n_sy
        to_plane(y, soon)
        held.append(y)
        if len(held) > LAG:
            to_plane(held.pop(0), later)
    for y in held:
        to_plane(y, later)

    tiles = n_sx // n_z
    far_first = sorted(range(1, n_px), key=lambda d: -min(d, n_px - d))
    reduce = []
    for step in range(n_z):
        passed = []
        for dz, dx in [(step, 0)] + [c for c in plane if c[0] == step and c[1]]:
            tile = at(-dz, -dx)
            if (dz, dx) != (0, 0):
                remote(pieces.at[tile], pieces.at[tile], {"sx": at(dz, dx)}, plane_sem[dz, dx]).wait_recv()
            passed.append((tile, send(pieces.at[tile], pieces.at[tile], {"sx": sibling})))
            merge_tile(pieces, gath_ref, tile)
        for tile, copy in passed:
            copy.wait_recv()
            merge_tile(pieces, gath_ref, tile + 1 - 2 * core)
        if step == 0:
            load.wait()
        which = (chip_z + n_z - step) % n_z
        basis_half = gath_ref[pl.ds(which * tiles, tiles)].reshape(half, pixels)

        def project(to):
            block = pat[pl.ds(pl.multiple_of(to * part, part), part), :]
            return lax.dot_general(block, basis_half, NT, preferred_element_type=f32)

        for d in far_first:
            part16[step, d] = project((px + d) % n_px).astype(bf16)
            reduce.append(send(part16.at[step, d], arrived.at[step, d], {"px": (px + d) % n_px}))
        own32[step] = project(px)

    for copy in load_maps:
        copy.wait()
    valid = jnp.transpose(valid_v[...].astype(f32))
    factor = (math.log2(math.e) / (2.0 * pix_total)) / jnp.transpose(strength_v[...])
    for b in range(n_px):
        for r in range(ROWS):
            size_col[b, cols * r:cols * (r + 1), 0:1] = valid[:, ROWS * b + r:ROWS * b + r + 1]
            size_col[b, cols * r:cols * (r + 1), 1:2] = factor[:, ROWS * b + r:ROWS * b + r + 1]

    def rows_of(which):
        return pl.ds(pl.multiple_of(pad + which * part, ROWS * EDGE), part)

    spread = []
    for step in range(n_z):
        which = (chip_z + n_z - step) % n_z
        for copy in reduce[step * len(far_first):(step + 1) * len(far_first)]:
            copy.wait_recv()
        total = own32[step]
        for d in range(1, n_px):
            total = total + arrived[step, d].astype(f32)
        mine = coeff.at[which, rows_of(px)]
        mine[...] = total.astype(bf16)
        spread += [(d, send(mine, mine, {"px": (px + d) % n_px})) for d in far_first]

    def sums(start, count):
        return jnp.concatenate([coeff[z, start:start + count] for z in range(n_z)], axis=1)

    def look(which):
        values = jnp.concatenate([coeff[z, rows_of(which)] for z in range(n_z)], axis=1)
        on = size_col[which, :, 0:1] > 0.5
        size = norms(values)
        size_col[which, :, 2:3] = size
        shown = jnp.where(on, values.astype(f32), FAR).astype(bf16)
        seen[which] = shown
        edges = jnp.dot(pick[...], shown, preferred_element_type=f32).astype(bf16)
        pack[0, which] = edges[:ROWS * EDGE]
        pack[1, which] = edges[ROWS * EDGE:]

    look(px)
    for d in far_first[::-1]:
        for e, copy in spread:
            if e == d:
                copy.wait_recv()
        look((px + n_px - d) % n_px)
    last = n_px - 1
    swap = [
        send(pack.at[0, 0], halo.at[n_px + 1, 0], {"sx": down, "sy": left}),
        send(pack.at[0, last], halo.at[0, 0], {"sx": up, "sy": left}),
        send(pack.at[1, 0], halo.at[n_px + 1, 1], {"sx": down, "sy": right}),
        send(pack.at[1, last], halo.at[0, 1], {"sx": up, "sy": right}),
        send(pack.at[0], halo.at[pl.ds(1, n_px), 0], {"sy": left}),
        send(pack.at[1], halo.at[pl.ds(1, n_px), 1], {"sy": right}),
        send(seen.at[0, pl.ds(0, pad)], rim.at[1], {"sx": down}),
        send(seen.at[last, pl.ds(part - pad, pad)], rim.at[0], {"sx": up}),
    ]

    for b in range(n_px):
        column = jnp.where(size_col[b, :, 0:1] > 0.5, size_col[b, :, 2:3], OFF)
        size_row[0:1, 128 * b + 128:128 * b + 128 + part] = across(column)
    n_wide = bias.shape[1]
    for b in range(n_px):
        center = sums(pad + part * b, part)
        lanes = 128 - pad + part * b
        sizes = size_row[0:1, lanes:lanes + n_wide]
        around_num[b], around_mass[b] = weigh(
            center, size_col[b, :, 2:3], size_col[b, :, 1:2], sums(part * b, n_wide), sizes, bias[...]
        )

    for copy in swap:
        copy.wait_recv()

    @pl.when(sx == 0)
    def _():
        rim[0] = jnp.full(rim.shape[1:], FAR, bf16)
        halo[0] = jnp.full(halo.shape[1:], FAR, bf16)

    @pl.when(sx == n_sx - 1)
    def _():
        rim[1] = jnp.full(rim.shape[1:], FAR, bf16)
        halo[n_px + 1] = jnp.full(halo.shape[1:], FAR, bf16)

    @pl.when(sy == 0)
    def _():
        halo[:, 1] = jnp.full((n_px + 2,) + halo.shape[2:], FAR, bf16)

    @pl.when(sy == n_sy - 1)
    def _():
        halo[:, 0] = jnp.full((n_px + 2,) + halo.shape[2:], FAR, bf16)

    def filled(values):
        return jnp.concatenate([values, jnp.zeros((128 - values.shape[0], rank), bf16)], axis=0)

    for b in range(n_px):
        center = sums(pad + part * b, part)
        around, outer = [filled(halo[b:b + 3].reshape(n_side, rank))], [bias_side[...]]
        if b == 0:
            around, outer = around + [filled(rim[0])], outer + [bias_top[...]]
        if b == last:
            around, outer = around + [filled(rim[1])], outer + [bias_low[...]]
        sizes = jnp.concatenate([across(norms(values)) for values in around], axis=1)
        summed, mass = weigh(
            center, size_col[b, :, 2:3], size_col[b, :, 1:2],
            jnp.concatenate(around, axis=0), sizes, jnp.concatenate(outer, axis=1),
        )
        summed = center.astype(f32) + around_num[b] + summed
        avg_ref[b] = (summed / (1.0 + around_mass[b] + mass)).astype(bf16)

    for dz, dx in plane:
        remote(pieces.at[sx], pieces.at[sx], {"sx": at(dz, dx)}, plane_sem[dz, dx]).wait_send()
    for copy in sent:
        copy.wait_send()


def merge_tile(pieces, gath_ref, tile):
    gath_ref[tile] = pieces[tile].reshape(gath_ref.shape[1:])


def rebuild(avg_ref, basis_ref, out_ref, made, sem):
    n_parts, _, n_lanes = made.shape
    copies = []
    for i in range(n_parts):
        lanes = pl.ds(i * n_lanes, n_lanes)
        product = jnp.dot(avg_ref[...], basis_ref[:, lanes], preferred_element_type=jnp.float32)
        made[i] = product.astype(made.dtype)
        copies.append(pltpu.make_async_copy(made.at[i], out_ref.at[:, lanes], sem.at[i]))
        copies[-1].start()
    for copy in copies:
        copy.wait()


def on_device(near, pix_total, patterns, basis, valid, strength):
    cells_x, cells_y, pixels = patterns.shape
    n_sx, n_sy, n_px = (lax.axis_size(name) for name in ("sx", "sy", "px"))
    depth = basis.shape[1]
    rank = depth * n_sx * n_sy
    part = cells_x * cells_y // n_px
    pad = RADIUS * cells_y
    bf16, f32 = jnp.bfloat16, jnp.float32
    n_z = near[0]
    half = rank // n_z
    n_copies = (n_sy - 1) + 2 * (n_sx // 2 - 1) + 1 + 2 * n_z * (n_px - 1) + 8
    n_wide = -(-(ROWS + 2 * RADIUS) * cells_y // 128) * 128
    vmem, hbm = pl.BlockSpec(memory_space=pltpu.VMEM), pl.BlockSpec(memory_space=pltpu.HBM)
    avg, gathered = pl.pallas_call(
        functools.partial(kernel, near, pix_total),
        out_shape=(
            jax.ShapeDtypeStruct((n_px, part, rank), bf16),
            jax.ShapeDtypeStruct((n_sx, depth * n_sy, pixels), bf16),
        ),
        in_specs=[hbm, hbm, hbm, hbm],
        out_specs=(vmem, vmem),
        scratch_shapes=[
            pltpu.VMEM((n_px * part, pixels), bf16),
            pltpu.VMEM((n_sx, n_sy, depth, pixels), bf16),
            pltpu.VMEM((n_z, part, half), f32),
            pltpu.VMEM((n_z, n_px, part, half), bf16),
            pltpu.VMEM((n_z, n_px, part, half), bf16),
            pltpu.VMEM((n_z, n_wide + (n_px - 1) * part, half), bf16),
            pltpu.VMEM((n_px, part, rank), bf16),
            pltpu.VMEM((2, pad, rank), bf16),
            pltpu.VMEM((n_px + 2, 2, ROWS * EDGE, rank), bf16),
            pltpu.VMEM((2, n_px, ROWS * EDGE, rank), bf16),
            pltpu.VMEM((2 * ROWS * EDGE, part), bf16),
            pltpu.VMEM((part, n_wide), f32),
            pltpu.VMEM((part, 128), f32),
            pltpu.VMEM((part, 128), f32),
            pltpu.VMEM((part, 128), f32),
            pltpu.VMEM((n_px, part, 128), f32),
            pltpu.VMEM((8, 128 + n_px * part + 512), f32),
            pltpu.VMEM((n_px, part, rank), f32),
            pltpu.VMEM((n_px, part, 1), f32),
            pltpu.VMEM(valid.shape, valid.dtype),
            pltpu.VMEM(strength.shape, strength.dtype),
            pltpu.SemaphoreType.DMA,
            pltpu.SemaphoreType.DMA,
            pltpu.SemaphoreType.DMA((2,)),
            pltpu.SemaphoreType.DMA((n_copies,)),
            pltpu.SemaphoreType.DMA((n_copies,)),
        ],
        compiler_params=pltpu.CompilerParams(collective_id=0, has_side_effects=True, vmem_limit_bytes=30 * 2**20),
    )(*[pltpu.with_memory_space_constraint(a, pltpu.HBM) for a in (patterns.reshape(cells_x * cells_y, pixels), basis.T, valid, strength)])
    n_cells, n_lanes = cells_x * cells_y, 256
    n_parts = pixels // n_lanes
    rebuilt = pl.pallas_call(
        rebuild,
        out_shape=jax.ShapeDtypeStruct((n_cells, pixels), bf16),
        in_specs=[vmem, vmem],
        out_specs=pl.BlockSpec(memory_space=pl.ANY),
        scratch_shapes=[pltpu.VMEM((n_parts, n_cells, n_lanes), bf16), pltpu.SemaphoreType.DMA((n_parts,))],
        compiler_params=pltpu.CompilerParams(vmem_limit_bytes=30 * 2**20),
    )(avg.reshape(n_cells, rank), gathered.reshape(rank, pixels))
    return rebuilt.reshape(cells_x, cells_y, pixels)


def solution(mesh, near=NEAR, pix_total=9216):
    return jax.shard_map(
        functools.partial(on_device, near, pix_total),
        mesh=mesh,
        in_specs=(P("sx", "sy", "px"), P("px", ("sx", "sy")), P("sx", "sy"), P("sx", "sy")),
        out_specs=P("sx", "sy", "px"),
        check_vma=False,
    )
```

```python
import functools
import math

import jax
import jax.numpy as jnp
from jax import lax
from jax.experimental import pallas as pl
from jax.experimental.pallas import tpu as pltpu
from jax.sharding import PartitionSpec as P

MESH = pl.DeviceIdType.MESH
RADIUS = 3
NEAR = (2, 4, 2)
FAR = 1e15
OFF = 1e30
EDGE = 4
LAG = 3
ROWS = 4
NT = (((1,), (1,)), ((), ()))


def across(column):
    n = column.shape[0]
    eye = lax.broadcasted_iota(jnp.int32, (n, n), 0) == lax.broadcasted_iota(jnp.int32, (n, n), 1)
    return jnp.sum(jnp.where(eye, column, 0.0), axis=0, keepdims=True)


def norms(values):
    wide = values.astype(jnp.float32)
    return jnp.sum(wide * wide, axis=1, keepdims=True)


def outside(d_row, d_col, known):
    near = (jnp.abs(d_row) <= RADIUS) & (jnp.abs(d_col) <= RADIUS) & known
    return jnp.where(near & ((d_row != 0) | (d_col != 0)), 0.0, OFF)


def weigh(center, size, scale, around, sizes, bias):
    inner = lax.dot_general(center, around, NT, preferred_element_type=jnp.float32)
    gap = jnp.maximum(size + sizes - 2.0 * inner, 0.0)
    weight = jnp.exp2(-(gap * scale + bias)).astype(jnp.bfloat16)
    summed = jnp.dot(weight, around, preferred_element_type=jnp.float32)
    return summed, jnp.sum(weight.astype(jnp.float32), axis=1, keepdims=True)


def kernel(
    near, pix_total, patterns_ref, basis_ref, valid_ref, strength_ref,
    avg_ref, gath_ref,
    pat, pieces, own32, part16, arrived, coeff, seen, rim, halo, pack, pick, bias, bias_top, bias_low, bias_side,
    size_col, size_row, around_num, around_mass, valid_v, strength_v,
    pat_sem, basis_sem, map_sem, send_sem, recv_sem,
):
    n_z, n_x, n_core = near
    n_sy, n_px = lax.axis_size("sy"), lax.axis_size("px")
    n_sx = n_z * n_x * n_core
    sx, sy, px = lax.axis_index("sx"), lax.axis_index("sy"), lax.axis_index("px")
    core = sx % n_core
    chip_x = (sx // n_core) % n_x
    chip_z = sx // (n_core * n_x)
    depth, pixels = pieces.shape[2], pieces.shape[3]
    part, half = own32.shape[1:]
    rank = n_z * half
    cols = part // ROWS
    n_rows = n_px * ROWS
    pad = RADIUS * cols
    f32, bf16 = jnp.float32, jnp.bfloat16

    def at(dz, dx):
        return (((chip_z + dz + n_z) % n_z) * n_x + (chip_x + dx + n_x) % n_x) * n_core + core

    sibling = sx + 1 - 2 * core
    up, down = (sx + 1) % n_sx, (sx + n_sx - 1) % n_sx
    right, left = (sy + 1) % n_sy, (sy + n_sy - 1) % n_sy
    hops = [min(d, n_x - d) for d in range(n_x)]
    plane = sorted(((dz, dx) for dx in range(n_x) for dz in range(n_z) if (dz, dx) != (0, 0)), key=lambda c: c[0] + hops[c[1]])

    load_basis = pltpu.make_async_copy(basis_ref, pieces.at[sx, sy], basis_sem)
    load_basis.start()
    load_maps = [
        pltpu.make_async_copy(valid_ref, valid_v, map_sem.at[0]),
        pltpu.make_async_copy(strength_ref, strength_v, map_sem.at[1]),
    ]
    for copy in load_maps:
        copy.start()
    load = pltpu.make_async_copy(patterns_ref, pat, pat_sem)
    load.start()

    partners = [{"sy": (sy + d) % n_sy} for d in range(1, n_sy)]
    partners += [{"sx": at(dz, dx)} for dz, dx in plane]
    partners += [{"px": (px + d) % n_px} for d in range(1, n_px)]
    partners += [{"sx": sibling}, {"sx": up}, {"sx": down}]
    partners += [{"sx": a, "sy": b} for a in (up, down) for b in (left, right)]

    def device(partner):
        return {"sx": sx, "sy": sy, "px": px, **partner}

    barrier = pltpu.get_barrier_semaphore()
    for partner in partners:
        pl.semaphore_signal(barrier, inc=1, device_id=device(partner), device_id_type=MESH)

    row = lax.broadcasted_iota(jnp.int32, pick.shape, 0)
    col = lax.broadcasted_iota(jnp.int32, pick.shape, 1)
    side, spot = row // (ROWS * EDGE), row % (ROWS * EDGE)
    pick[...] = jnp.where(col == (spot // EDGE) * cols + spot % EDGE + side * (cols - EDGE), 1.0, 0.0).astype(bf16)

    mine = lax.broadcasted_iota(jnp.int32, (part, 128), 0)
    lane = lax.broadcasted_iota(jnp.int32, (part, 128), 1)
    my_row, my_col = mine // cols, mine % cols
    n_mid = (ROWS + 2 * RADIUS) * cols
    n_side = 3 * 2 * ROWS * EDGE
    for k in range(bias.shape[1] // 128):
        spot = lane + 128 * k
        bias[:, 128 * k:128 * (k + 1)] = outside(spot // cols - RADIUS - my_row, spot % cols - my_col, spot < n_mid)
    spot = lane % (ROWS * EDGE)
    side_row = (lane // (2 * ROWS * EDGE)) * ROWS + spot // EDGE - ROWS
    side_col = spot % EDGE + jnp.where((lane // (ROWS * EDGE)) % 2 == 0, cols, -EDGE)
    bias_side[...] = outside(side_row - my_row, side_col - my_col, lane < n_side)
    bias_top[...] = outside(lane // cols - RADIUS - my_row, lane % cols - my_col, lane < pad)
    bias_low[...] = outside(lane // cols + ROWS - my_row, lane % cols - my_col, lane < pad)
    n_tail = coeff.shape[1] - pad - n_px * part
    coeff[:, 0:pad] = jnp.zeros((n_z, pad, half), bf16)
    coeff[:, pad + n_px * part:] = jnp.zeros((n_z, n_tail, half), bf16)
    size_row[...] = jnp.full(size_row.shape, OFF, f32)

    load_basis.wait()
    pl.semaphore_wait(barrier, len(partners))

    sent = []
    n_send = [0]

    def remote(src, dst, partner, k):
        return pltpu.make_async_remote_copy(
            src_ref=src, dst_ref=dst, send_sem=send_sem.at[k], recv_sem=recv_sem.at[k],
            device_id=device(partner), device_id_type=MESH,
        )

    def fresh():
        n_send[0] += 1
        return n_send[0] - 1

    def send(src, dst, partner):
        copy = remote(src, dst, partner, fresh())
        copy.start()
        sent.append(copy)
        return copy

    order = sorted(range(1, n_sy), key=lambda d: -min(d, n_sy - d))
    along = {d: send(pieces.at[sx, sy], pieces.at[sx, sy], {"sy": (sy + d) % n_sy}) for d in order}
    plane_sem = {c: fresh() for c in plane}

    def to_plane(y, targets):
        for dz, dx in targets:
            remote(pieces.at[sx, y], pieces.at[sx, y], {"sx": at(dz, dx)}, plane_sem[dz, dx]).start()

    soon = [c for c in plane[::-1] if c[0] == 0 or c[1] == 0]
    later = [c for c in plane[::-1] if c not in soon]
    held = []
    for d in [0] + order[::-1]:
        if d:
            along[d].wait_recv()
        y = (sy + n_sy - d) % n_sy
        to_plane(y, soon)
        held.append(y)
        if len(held) > LAG:
            to_plane(held.pop(0), later)
    for y in held:
        to_plane(y, later)

    tiles = n_sx // n_z
    far_first = sorted(range(1, n_px), key=lambda d: -min(d, n_px - d))
    reduce = []
    for step in range(n_z):
        passed = []
        for dz, dx in [(step, 0)] + [c for c in plane if c[0] == step and c[1]]:
            tile = at(-dz, -dx)
            if (dz, dx) != (0, 0):
                remote(pieces.at[tile], pieces.at[tile], {"sx": at(dz, dx)}, plane_sem[dz, dx]).wait_recv()
            passed.append((tile, send(pieces.at[tile], pieces.at[tile], {"sx": sibling})))
        for tile, _ in passed:
            merge_tile(pieces, gath_ref, tile)
        for tile, copy in passed:
            copy.wait_recv()
            merge_tile(pieces, gath_ref, tile + 1 - 2 * core)
        if step == 0:
            load.wait()
        which = (chip_z + n_z - step) % n_z
        basis_half = gath_ref[pl.ds(which * tiles, tiles)].reshape(half, pixels)

        def project(to):
            block = pat[pl.ds(pl.multiple_of(to * part, part), part), :]
            return lax.dot_general(block, basis_half, NT, preferred_element_type=f32)

        for d in far_first:
            part16[step, d] = project((px + d) % n_px).astype(bf16)
            reduce.append(send(part16.at[step, d], arrived.at[step, d], {"px": (px + d) % n_px}))
        own32[step] = project(px)

    for copy in load_maps:
        copy.wait()
    valid = jnp.transpose(valid_v[...].astype(f32))
    factor = (math.log2(math.e) / (2.0 * pix_total)) / jnp.transpose(strength_v[...])
    for b in range(n_px):
        for r in range(ROWS):
            size_col[b, cols * r:cols * (r + 1), 0:1] = valid[:, ROWS * b + r:ROWS * b + r + 1]
            size_col[b, cols * r:cols * (r + 1), 1:2] = factor[:, ROWS * b + r:ROWS * b + r + 1]

    def rows_of(which):
        return pl.ds(pl.multiple_of(pad + which * part, ROWS * EDGE), part)

    spread = []
    for step in range(n_z):
        which = (chip_z + n_z - step) % n_z
        for copy in reduce[step * len(far_first):(step + 1) * len(far_first)]:
            copy.wait_recv()
        total = own32[step]
        for d in range(1, n_px):
            total = total + arrived[step, d].astype(f32)
        mine = coeff.at[which, rows_of(px)]
        mine[...] = total.astype(bf16)
        spread += [(d, send(mine, mine, {"px": (px + d) % n_px})) for d in far_first]

    def sums(start, count):
        return jnp.concatenate([coeff[z, start:start + count] for z in range(n_z)], axis=1)

    def look(which):
        values = jnp.concatenate([coeff[z, rows_of(which)] for z in range(n_z)], axis=1)
        on = size_col[which, :, 0:1] > 0.5
        shown = jnp.where(on, values.astype(f32), FAR).astype(bf16)
        seen[which] = shown
        edges = jnp.dot(pick[...], shown, preferred_element_type=f32).astype(bf16)
        pack[0, which] = edges[:ROWS * EDGE]
        pack[1, which] = edges[ROWS * EDGE:]
        swap.append(send(pack.at[0, which], halo.at[which + 1, 0], {"sy": left}))
        swap.append(send(pack.at[1, which], halo.at[which + 1, 1], {"sy": right}))

    swap = []
    look(px)
    for d in far_first[::-1]:
        for e, copy in spread:
            if e == d:
                copy.wait_recv()
        look((px + n_px - d) % n_px)
    last = n_px - 1
    swap += [
        send(pack.at[0, 0], halo.at[n_px + 1, 0], {"sx": down, "sy": left}),
        send(pack.at[0, last], halo.at[0, 0], {"sx": up, "sy": left}),
        send(pack.at[1, 0], halo.at[n_px + 1, 1], {"sx": down, "sy": right}),
        send(pack.at[1, last], halo.at[0, 1], {"sx": up, "sy": right}),
        send(seen.at[0, pl.ds(0, pad)], rim.at[1], {"sx": down}),
        send(seen.at[last, pl.ds(part - pad, pad)], rim.at[0], {"sx": up}),
    ]

    for b in range(n_px):
        size_col[b, :, 2:3] = norms(sums(pad + part * b, part))
        column = jnp.where(size_col[b, :, 0:1] > 0.5, size_col[b, :, 2:3], OFF)
        size_row[0:1, 128 * b + 128:128 * b + 128 + part] = across(column)
    n_wide = bias.shape[1]
    for b in range(n_px):
        center = sums(pad + part * b, part)
        lanes = 128 - pad + part * b
        sizes = size_row[0:1, lanes:lanes + n_wide]
        around_num[b], around_mass[b] = weigh(
            center, size_col[b, :, 2:3], size_col[b, :, 1:2], sums(part * b, n_wide), sizes, bias[...]
        )

    for copy in swap:
        copy.wait_recv()

    @pl.when(sx == 0)
    def _():
        rim[0] = jnp.full(rim.shape[1:], FAR, bf16)
        halo[0] = jnp.full(halo.shape[1:], FAR, bf16)

    @pl.when(sx == n_sx - 1)
    def _():
        rim[1] = jnp.full(rim.shape[1:], FAR, bf16)
        halo[n_px + 1] = jnp.full(halo.shape[1:], FAR, bf16)

    @pl.when(sy == 0)
    def _():
        halo[:, 1] = jnp.full((n_px + 2,) + halo.shape[2:], FAR, bf16)

    @pl.when(sy == n_sy - 1)
    def _():
        halo[:, 0] = jnp.full((n_px + 2,) + halo.shape[2:], FAR, bf16)

    def filled(values):
        return jnp.concatenate([values, jnp.zeros((128 - values.shape[0], rank), bf16)], axis=0)

    for b in range(n_px):
        center = sums(pad + part * b, part)
        around, outer = [filled(halo[b:b + 3].reshape(n_side, rank))], [bias_side[...]]
        if b == 0:
            around, outer = around + [filled(rim[0])], outer + [bias_top[...]]
        if b == last:
            around, outer = around + [filled(rim[1])], outer + [bias_low[...]]
        sizes = jnp.concatenate([across(norms(values)) for values in around], axis=1)
        summed, mass = weigh(
            center, size_col[b, :, 2:3], size_col[b, :, 1:2],
            jnp.concatenate(around, axis=0), sizes, jnp.concatenate(outer, axis=1),
        )
        summed = center.astype(f32) + around_num[b] + summed
        avg_ref[b] = (summed / (1.0 + around_mass[b] + mass)).astype(bf16)

    for dz, dx in plane:
        remote(pieces.at[sx], pieces.at[sx], {"sx": at(dz, dx)}, plane_sem[dz, dx]).wait_send()
    for copy in sent:
        copy.wait_send()


def merge_tile(pieces, gath_ref, tile):
    gath_ref[tile] = pieces[tile].reshape(gath_ref.shape[1:])


def rebuild(avg_ref, basis_ref, out_ref, made, sem):
    n_parts, _, n_lanes = made.shape
    copies = []
    for i in range(n_parts):
        lanes = pl.ds(i * n_lanes, n_lanes)
        product = jnp.dot(avg_ref[...], basis_ref[:, lanes], preferred_element_type=jnp.float32)
        made[i] = product.astype(made.dtype)
        copies.append(pltpu.make_async_copy(made.at[i], out_ref.at[:, lanes], sem.at[i]))
        copies[-1].start()
    for copy in copies:
        copy.wait()


def on_device(near, pix_total, patterns, basis, valid, strength):
    cells_x, cells_y, pixels = patterns.shape
    n_sx, n_sy, n_px = (lax.axis_size(name) for name in ("sx", "sy", "px"))
    depth = basis.shape[1]
    rank = depth * n_sx * n_sy
    part = cells_x * cells_y // n_px
    pad = RADIUS * cells_y
    bf16, f32 = jnp.bfloat16, jnp.float32
    n_z = near[0]
    half = rank // n_z
    n_copies = (n_sy - 1) + 2 * (n_sx // 2 - 1) + 1 + 2 * n_z * (n_px - 1) + 6 + 2 * n_px
    n_wide = -(-(ROWS + 2 * RADIUS) * cells_y // 128) * 128
    vmem, hbm = pl.BlockSpec(memory_space=pltpu.VMEM), pl.BlockSpec(memory_space=pltpu.HBM)
    avg, gathered = pl.pallas_call(
        functools.partial(kernel, near, pix_total),
        out_shape=(
            jax.ShapeDtypeStruct((n_px, part, rank), bf16),
            jax.ShapeDtypeStruct((n_sx, depth * n_sy, pixels), bf16),
        ),
        in_specs=[hbm, hbm, hbm, hbm],
        out_specs=(vmem, vmem),
        scratch_shapes=[
            pltpu.VMEM((n_px * part, pixels), bf16),
            pltpu.VMEM((n_sx, n_sy, depth, pixels), bf16),
            pltpu.VMEM((n_z, part, half), f32),
            pltpu.VMEM((n_z, n_px, part, half), bf16),
            pltpu.VMEM((n_z, n_px, part, half), bf16),
            pltpu.VMEM((n_z, n_wide + (n_px - 1) * part, half), bf16),
            pltpu.VMEM((n_px, part, rank), bf16),
            pltpu.VMEM((2, pad, rank), bf16),
            pltpu.VMEM((n_px + 2, 2, ROWS * EDGE, rank), bf16),
            pltpu.VMEM((2, n_px, ROWS * EDGE, rank), bf16),
            pltpu.VMEM((2 * ROWS * EDGE, part), bf16),
            pltpu.VMEM((part, n_wide), f32),
            pltpu.VMEM((part, 128), f32),
            pltpu.VMEM((part, 128), f32),
            pltpu.VMEM((part, 128), f32),
            pltpu.VMEM((n_px, part, 128), f32),
            pltpu.VMEM((8, 128 + n_px * part + 512), f32),
            pltpu.VMEM((n_px, part, rank), f32),
            pltpu.VMEM((n_px, part, 1), f32),
            pltpu.VMEM(valid.shape, valid.dtype),
            pltpu.VMEM(strength.shape, strength.dtype),
            pltpu.SemaphoreType.DMA,
            pltpu.SemaphoreType.DMA,
            pltpu.SemaphoreType.DMA((2,)),
            pltpu.SemaphoreType.DMA((n_copies,)),
            pltpu.SemaphoreType.DMA((n_copies,)),
        ],
        compiler_params=pltpu.CompilerParams(collective_id=0, has_side_effects=True, vmem_limit_bytes=30 * 2**20),
    )(*[pltpu.with_memory_space_constraint(a, pltpu.HBM) for a in (patterns.reshape(cells_x * cells_y, pixels), basis.T, valid, strength)])
    n_cells, n_lanes = cells_x * cells_y, 256
    n_parts = pixels // n_lanes
    rebuilt = pl.pallas_call(
        rebuild,
        out_shape=jax.ShapeDtypeStruct((n_cells, pixels), bf16),
        in_specs=[vmem, vmem],
        out_specs=pl.BlockSpec(memory_space=pl.ANY),
        scratch_shapes=[pltpu.VMEM((n_parts, n_cells, n_lanes), bf16), pltpu.SemaphoreType.DMA((n_parts,))],
        compiler_params=pltpu.CompilerParams(vmem_limit_bytes=30 * 2**20),
    )(avg.reshape(n_cells, rank), gathered.reshape(rank, pixels))
    return rebuilt.reshape(cells_x, cells_y, pixels)


def solution(mesh, near=NEAR, pix_total=9216):
    return jax.shard_map(
        functools.partial(on_device, near, pix_total),
        mesh=mesh,
        in_specs=(P("sx", "sy", "px"), P("px", ("sx", "sy")), P("sx", "sy"), P("sx", "sy")),
        out_specs=P("sx", "sy", "px"),
        check_vma=False,
    )
```
